8 devices in a mesh: dp: 2 (over y, z), tp: 4 (over x, core).
Axes of the slice: x: 2, y: 2, z: 1, core: 2. Of those that a mesh axis runs over, the one named last changes fastest.
Arguments:
- x: bfloat16 [256, 12288], P('dp'), parts along dimension 0
- w_gate: bfloat16 [12288, 28672], P(None, 'tp')
- w_up: bfloat16 [12288, 28672], P(None, 'tp')
- w_down: bfloat16 [28672, 12288], P('tp')
Outputs:
- output: bfloat16 [256, 12288], P('dp'), parts along dimension 0
There are 2 independent parts. The reference program is written for one: setup_inputs(seed, part) draws one part's arguments, and reference() takes and returns one part's arrays. A program takes and returns all parts, laid end to end along the dimension named above; an argument that names none is the same for every part.
All inputs are finite; a program needn't handle non-finite values.
Results may differ from the reference program's by a relative error of at most 0.016.
Values are sent between devices in bfloat16 or wider.
A program may use at most 2 GiB of HBM per device.

```python
import jax
import jax.numpy as jnp

ROWS = 128
D = 12288
FF = 28672


def setup_inputs(seed: int = 0, part: int = 0) -> dict:
    kx, kg, ku, kd = jax.random.split(jax.random.key(seed), 4)
    drawn = {
        "x": jax.random.normal(jax.random.fold_in(kx, part), (ROWS, D), jnp.float32),
        "w_gate": jax.random.normal(kg, (D, FF), jnp.float32) * D**-0.5,
        "w_up": jax.random.normal(ku, (D, FF), jnp.float32) * D**-0.5,
        "w_down": jax.random.normal(kd, (FF, D), jnp.float32) * FF**-0.5,
    }
    return {k: v.astype(jnp.bfloat16) for k, v in drawn.items()}


def reference(x, w_gate, w_up, w_down):
    gate = jnp.dot(x, w_gate, preferred_element_type=jnp.float32)
    up = jnp.dot(x, w_up, preferred_element_type=jnp.float32)
    hidden = (jax.nn.silu(gate) * up).astype(jnp.bfloat16)
    return jnp.dot(hidden, w_down, preferred_element_type=jnp.float32).astype(jnp.bfloat16)
```

```python
import functools

import jax
import jax.numpy as jnp
from jax import lax
from jax.experimental import pallas as pl
from jax.experimental.pallas import tpu as pltpu
from jax.sharding import PartitionSpec as P

MESH = pl.DeviceIdType.MESH
F32 = jnp.float32
BF16 = jnp.bfloat16

KC = 512
NC = 512
SLOTS = 8
LAG_B, LAG_C, LAG_D = 1, 4, 7


def kernel(
    x_ref, wg_ref, wu_ref, wd_ref, y_ref,
    xb, w, acc_g, acc_u, hid, keep, mine, a_out, a_in, b_out, b_in, c_out, c_in, fin,
    x_load, x_send, x_recv, f_send, f_recv, w_sem,
    a_send, a_recv, b_send, b_recv, c_send, c_recv, d_send, d_recv, d_local,
):
    rows, depth = x_ref.shape
    steps = depth // KC
    blocks = w.shape[1]
    half_ff = blocks * NC
    half = NC // 2
    side = depth // 2
    chunks = side // half
    part = rows // 2

    dp, tp = lax.axis_index("dp"), lax.axis_index("tp")
    core = lax.rem(tp, 2)
    over_core = {"dp": dp, "tp": tp + 1 - 2 * core}
    over_y = {"dp": 1 - dp, "tp": tp}
    over_x = {"dp": dp, "tp": lax.rem(tp + 2, 4)}

    def load_x(s):
        cols = pl.ds(pl.multiple_of(s * KC, KC), KC)
        return pltpu.make_async_copy(x_ref.at[:, cols], xb.at[s, pl.ds(0, rows), :], x_load.at[s])

    def send_x(s):
        src = xb.at[s, pl.ds(pl.multiple_of(part * core, part), part), :]
        dst = xb.at[s, pl.ds(pl.multiple_of(rows + part * core, part), part), :]
        return pltpu.make_async_remote_copy(
            src, dst, x_send.at[s], x_recv.at[s], device_id=over_y, device_id_type=MESH)

    def forward_x(s):
        ref = xb.at[s, pl.ds(pl.multiple_of(rows + part * core, part), part), :]
        return pltpu.make_async_remote_copy(
            ref, ref, f_send.at[s], f_recv.at[s], device_id=over_core, device_id_type=MESH)

    def load_in(src_ref, s, slot):
        for j in range(blocks):
            cols = pl.ds(pl.multiple_of(half_ff * dp + j * NC, NC), NC)
            pltpu.make_async_copy(
                src_ref.at[pl.ds(pl.multiple_of(s * KC, KC), KC), cols], w.at[slot, j], w_sem.at[slot]).start()

    def load_down(n, slot):
        for i, owner in enumerate((core, 1 - core)):
            cols = pl.ds(pl.multiple_of(side * owner + half * n, half), half)
            pltpu.make_async_copy(
                wd_ref.at[pl.ds(blocks * dp, blocks), :, cols],
                w.at[slot, :, :, pl.ds(i * half, half)], w_sem.at[slot]).start()

    def wait_w(slot):
        pltpu.make_async_copy(w.at[slot], w.at[slot], w_sem.at[slot]).wait()

    def a_copy(n):
        return pltpu.make_async_remote_copy(
            a_out.at[n], a_in.at[n], a_send.at[n], a_recv.at[n], device_id=over_core, device_id_type=MESH)

    def b_copy(n):
        return pltpu.make_async_remote_copy(
            b_out.at[n], b_in.at[n], b_send.at[n], b_recv.at[n], device_id=over_y, device_id_type=MESH)

    def c_copy(n):
        return pltpu.make_async_remote_copy(
            c_out.at[n], c_in.at[n], c_send.at[n], c_recv.at[n], device_id=over_x, device_id_type=MESH)

    def d_cols(owner, n):
        return y_ref.at[:, pl.ds(pl.multiple_of(side * owner + half * n, half), half)]

    def d_copy(n):
        return pltpu.make_async_remote_copy(
            fin.at[n], d_cols(core, n), d_send.at[n], d_recv.at[n], device_id=over_core, device_id_type=MESH)

    def d_keep(n):
        return pltpu.make_async_copy(fin.at[n], d_cols(core, n), d_local.at[n])

    def loop(lo, hi, body):
        def run(i, carry):
            body(i)
            return carry

        lax.fori_loop(lo, hi, run, 0)

    loop(0, steps, lambda s: load_x(s).start())
    for s in range(SLOTS // 2):
        load_in(wg_ref, s, 2 * s)
        load_in(wu_ref, s, 2 * s + 1)
    barrier = pltpu.get_barrier_semaphore()
    for other in (over_core, over_y, over_x):
        pl.semaphore_signal(barrier, inc=1, device_id=other, device_id_type=MESH)
    pl.semaphore_wait(barrier, 3)

    def first(s):
        load_x(s).wait()
        send_x(s).start()

    loop(0, steps, first)
    acc_g[...] = jnp.zeros_like(acc_g)
    acc_u[...] = jnp.zeros_like(acc_u)
    send_x(0).wait_recv()
    forward_x(0).start()

    def refill(s, slot, src_ref, odd):
        @pl.when(s + SLOTS // 2 < steps)
        def _():
            load_in(src_ref, s + SLOTS // 2, slot)

        @pl.when(s + SLOTS // 2 >= steps)
        def _():
            load_down(2 * (s + SLOTS // 2 - steps) + odd, slot)

    def project(s):
        @pl.when(s + 1 < steps)
        def _():
            send_x(s + 1).wait_recv()
            forward_x(s + 1).start()

        forward_x(s).wait_recv()
        for odd, (src_ref, acc) in enumerate(((wg_ref, acc_g), (wu_ref, acc_u))):
            slot = lax.rem(2 * s + odd, SLOTS)
            wait_w(slot)
            for j in range(blocks):
                acc[j] += jnp.dot(xb[s], w[slot, j], preferred_element_type=F32)
            refill(s, slot, src_ref, odd)

    loop(0, steps, project)

    for j in range(blocks):
        hid[:, j * NC:(j + 1) * NC] = (jax.nn.silu(acc_g[j]) * acc_u[j]).astype(BF16)

    def finish(n):
        @pl.when(n < chunks)
        def _():
            slot = lax.rem(n, SLOTS)
            wait_w(slot)
            term = jnp.dot(hid[...], w[slot].reshape(half_ff, NC), preferred_element_type=F32)
            a_out[n] = term[:, half:].astype(BF16)
            keep[lax.rem(n, LAG_B + 1)] = term[:, :half]
            a_copy(n).start()

            @pl.when(n + SLOTS < chunks)
            def _():
                load_down(n + SLOTS, slot)

        b = n - LAG_B

        @pl.when((b >= 0) & (b < chunks))
        def _():
            a_copy(b).wait_recv()
            total = keep[lax.rem(b, LAG_B + 1)] + a_in[b].astype(F32)
            b_out[b] = total[rows:].astype(BF16)
            mine[b] = total[:rows]
            b_copy(b).start()

        c = n - LAG_C

        @pl.when((c >= 0) & (c < chunks))
        def _():
            b_copy(c).wait_recv()
            c_out[c] = (mine[c] + b_in[c].astype(F32)).astype(BF16)
            c_copy(c).start()

        d = n - LAG_D

        @pl.when(d >= 0)
        def _():
            c_copy(d).wait_recv()
            fin[d] = (c_out[d].astype(F32) + c_in[d].astype(F32)).astype(BF16)
            d_copy(d).start()
            d_keep(d).start()

    loop(0, chunks + LAG_D, finish)

    def last_x(s):
        send_x(s).wait_send()
        forward_x(s).wait_send()

    def last(n):
        a_copy(n).wait_send()
        b_copy(n).wait_send()
        c_copy(n).wait_send()
        d_keep(n).wait()
        d_copy(n).wait()

    loop(0, steps, last_x)
    loop(0, chunks, last)


def solution(mesh):
    def step(x, w_gate, w_up, w_down):
        rows, depth = x.shape
        ff = w_gate.shape[1]
        blocks = ff // 2 // NC
        steps = depth // KC
        half = NC // 2
        chunks = depth // NC
        dma = pltpu.SemaphoreType.DMA
        hbm = pl.BlockSpec(memory_space=pl.ANY)
        return pl.pallas_call(
            kernel,
            out_shape=jax.ShapeDtypeStruct((rows, depth), BF16),
            in_specs=[hbm] * 4,
            out_specs=hbm,
            scratch_shapes=[
                pltpu.VMEM((steps, 2 * rows, KC), BF16),
                pltpu.VMEM((SLOTS, blocks, KC, NC), BF16),
                pltpu.VMEM((blocks, 2 * rows, NC), F32),
                pltpu.VMEM((blocks, 2 * rows, NC), F32),
                pltpu.VMEM((2 * rows, blocks * NC), BF16),
                pltpu.VMEM((LAG_B + 1, 2 * rows, half), F32),
                pltpu.VMEM((chunks, rows, half), F32),
                pltpu.VMEM((chunks, 2 * rows, half), BF16),
                pltpu.VMEM((chunks, 2 * rows, half), BF16),
                pltpu.VMEM((chunks, rows, half), BF16),
                pltpu.VMEM((chunks, rows, half), BF16),
                pltpu.VMEM((chunks, rows, half), BF16),
                pltpu.VMEM((chunks, rows, half), BF16),
                pltpu.VMEM((chunks, rows, half), BF16),
                dma((steps,)), dma((steps,)), dma((steps,)), dma((steps,)), dma((steps,)), dma((SLOTS,)),
                dma((chunks,)), dma((chunks,)), dma((chunks,)), dma((chunks,)), dma((chunks,)), dma((chunks,)),
                dma((chunks,)), dma((chunks,)), dma((chunks,)),
            ],
            compiler_params=pltpu.CompilerParams(
                collective_id=0, has_side_effects=True, vmem_limit_bytes=67_000_000),
        )(x, w_gate, w_up, w_down.reshape(ff // NC, NC, depth))

    return jax.shard_map(
        step,
        mesh=mesh,
        in_specs=(P("dp", None), P(None, "tp"), P(None, "tp"), P("tp", None)),
        out_specs=P("dp", None),
        check_vma=False,
    )
```

```python
import functools

import jax
import jax.numpy as jnp
from jax import lax
from jax.experimental import pallas as pl
from jax.experimental.pallas import tpu as pltpu
from jax.sharding import PartitionSpec as P

MESH = pl.DeviceIdType.MESH
F32 = jnp.float32
BF16 = jnp.bfloat16

KC = 512
NC = 512
SUB = 256
PER = NC // (2 * SUB)
SLOTS = 10
EARLY = 2
SINGLES = 6
LAG_B, LAG_C, LAG_D = 1, 4, 7
RING_A, RING_B, RING_C = 4, 8, 8


def kernel(
    x_ref, wg_ref, wu_ref, wd_ref, y_ref,
    xb, w, acc_g, acc_u, hid, a_in, b_in, c_in,
    x_load, x_send, x_recv, f_send, f_recv, w_sem,
    a_send, a_recv, b_send, b_recv, c_send, c_recv, d_send, d_recv,
):
    rows, depth = x_ref.shape
    steps = depth // KC
    blocks = w.shape[1]
    half_ff = blocks * NC
    side = depth // 2
    units = depth // NC
    part = rows // 2
    both = (0, 2 * rows)

    dp, tp = lax.axis_index("dp"), lax.axis_index("tp")
    core = lax.rem(tp, 2)
    over_core = {"dp": dp, "tp": tp + 1 - 2 * core}
    over_y = {"dp": 1 - dp, "tp": tp}
    over_x = {"dp": dp, "tp": lax.rem(tp + 2, 4)}

    def load_x(s):
        cols = pl.ds(pl.multiple_of(s * KC, KC), KC)
        which = (s >= SINGLES).astype(jnp.int32)
        return pltpu.make_async_copy(x_ref.at[:, cols], xb.at[s, pl.ds(0, rows), :], x_load.at[which])

    def loaded_x(first, count, which):
        ref = xb.at[pl.ds(first, count), pl.ds(0, rows), :]
        pltpu.make_async_copy(ref, ref, x_load.at[which]).wait()

    def x_part(base, s, count):
        return xb.at[pl.ds(s, count), pl.ds(pl.multiple_of(base + part * core, part), part), :]

    def x_sem(s, count):
        return s if count == 1 else SINGLES + (s - SINGLES) // 2

    def send_x(s, count):
        return pltpu.make_async_remote_copy(
            x_part(0, s, count), x_part(rows, s, count), x_send.at[0], x_recv.at[x_sem(s, count)],
            device_id=over_y, device_id_type=MESH)

    def forward_x(s, count):
        ref = x_part(rows, s, count)
        return pltpu.make_async_remote_copy(
            ref, ref, f_send.at[0], f_recv.at[x_sem(s, count)], device_id=over_core, device_id_type=MESH)

    def load_in(src_ref, s, slot):
        for j in range(blocks):
            cols = pl.ds(pl.multiple_of(half_ff * dp + j * NC, NC), NC)
            pltpu.make_async_copy(
                src_ref.at[pl.ds(pl.multiple_of(s * KC, KC), KC), cols], w.at[slot, j], w_sem.at[slot]).start()

    def load_down(n, slot):
        for sub in range(PER):
            for i, owner in enumerate((core, 1 - core)):
                cols = pl.ds(pl.multiple_of(side * owner + PER * SUB * n + SUB * sub, SUB), SUB)
                pltpu.make_async_copy(
                    wd_ref.at[pl.ds(blocks * dp, blocks), :, cols],
                    w.at[slot, :, :, pl.ds((2 * sub + i) * SUB, SUB)], w_sem.at[slot]).start()

    def wait_w(slot):
        pltpu.make_async_copy(w.at[slot], w.at[slot], w_sem.at[slot]).wait()

    def a_out(n, sub):
        return xb.at[n, :, pl.ds(2 * SUB * sub, SUB)]

    def b_out(n, sub):
        return xb.at[n, pl.ds(0, rows), pl.ds(2 * SUB * sub + SUB, SUB)]

    def c_out(n, sub):
        return xb.at[n, pl.ds(rows, rows), pl.ds(2 * SUB * sub + SUB, SUB)]

    def keep(n, sub):
        return acc_u.at[lax.rem(n, blocks), :, pl.ds(SUB * sub, SUB)]

    def mine(n, sub):
        return acc_g.at[lax.rem(n, blocks), pl.ds(0, rows), pl.ds(SUB * sub, SUB)]

    def a_copy(n, sub):
        m = PER * n + sub
        return pltpu.make_async_remote_copy(
            a_out(n, sub), a_in.at[m], a_send.at[0], a_recv.at[lax.rem(m, RING_A)],
            device_id=over_core, device_id_type=MESH)

    def b_copy(n, sub):
        m = PER * n + sub
        return pltpu.make_async_remote_copy(
            b_out(n, sub), b_in.at[m], b_send.at[0], b_recv.at[lax.rem(m, RING_B)],
            device_id=over_y, device_id_type=MESH)

    def c_copy(n, sub):
        m = PER * n + sub
        return pltpu.make_async_remote_copy(
            c_out(n, sub), c_in.at[m], c_send.at[0], c_recv.at[lax.rem(m, RING_C)],
            device_id=over_x, device_id_type=MESH)

    def d_cols(n, sub):
        return y_ref.at[:, pl.ds(pl.multiple_of(side * core + PER * SUB * n + SUB * sub, SUB), SUB)]

    def d_copy(n, sub):
        ref = d_cols(n, sub)
        return pltpu.make_async_remote_copy(
            ref, ref, d_send.at[0], d_recv.at[0], device_id=over_core, device_id_type=MESH)

    def loop(lo, hi, body):
        def run(i, carry):
            body(i)
            return carry

        lax.fori_loop(lo, hi, run, 0)

    barrier = pltpu.get_barrier_semaphore()
    for other in (over_core, over_y, over_x):
        pl.semaphore_signal(barrier, inc=1, device_id=other, device_id_type=MESH)
    loop(0, steps, lambda s: load_x(s).start())

    ins = ((wg_ref, acc_g), (wu_ref, acc_u))

    def slot_in(s, which):
        return lax.rem(2 * s + which, SLOTS)

    def slot_down(n):
        return lax.rem(2 * steps + n, SLOTS)

    for s in range(SLOTS // 2):
        for which in range(2):
            load_in(ins[which][0], s, slot_in(s, which))
    acc_g[...] = jnp.zeros_like(acc_g)
    acc_u[...] = jnp.zeros_like(acc_u)
    pl.semaphore_wait(barrier, 3)

    loaded_x(0, SINGLES, 0)
    loop(0, SINGLES, lambda s: send_x(s, 1).start())
    loaded_x(SINGLES, steps - SINGLES, 1)
    loop(SINGLES // 2, steps // 2, lambda step: send_x(2 * step, 2).start())

    def project(s, count, span, wait=True, free=True, last=False):
        lo, size = span
        if wait:
            for which in range(2):
                for i in range(count):
                    wait_w(slot_in(s + i, which))
        for which, (src_ref, acc) in enumerate(ins):
            for j in range(blocks):
                total = acc[j, lo:lo + size, :]
                for i in range(count):
                    total += jnp.dot(
                        xb[s + i, lo:lo + size, :], w[slot_in(s + i, which), j], preferred_element_type=F32)
                acc[j, lo:lo + size, :] = total
            for i in range(count if free else 0):
                ahead = s + i + SLOTS // 2
                slot = slot_in(s + i, which)
                if not last:
                    load_in(src_ref, ahead, slot)
                    continue

                @pl.when(ahead < steps)
                def _():
                    load_in(src_ref, ahead, slot)

                @pl.when(ahead >= steps)
                def _():
                    load_down(2 * (ahead - steps) + which, slot)

    def take_x(s, count):
        send_x(s, count).wait_recv()
        forward_x(s, count).start()

    loop(0, EARLY, lambda s: project(s, 1, (0, rows), free=False))
    take_x(0, 1)

    def late(s):
        take_x(s + 1, 1)
        forward_x(s, 1).wait_recv()
        project(s, 1, (rows, rows), wait=False)

    loop(0, EARLY, late)

    def single(s):
        @pl.when(s + 1 < SINGLES)
        def _():
            take_x(s + 1, 1)

        @pl.when(s + 1 == SINGLES)
        def _():
            take_x(SINGLES, 2)

        forward_x(s, 1).wait_recv()
        project(s, 1, both)

    loop(EARLY, SINGLES, single)

    def double(s, last):
        @pl.when(s + 2 < steps)
        def _():
            take_x(s + 2, 2)

        forward_x(s, 2).wait_recv()
        project(s, 2, both, last=last)

    tail = (steps - SLOTS // 2) // 2 * 2
    loop(SINGLES // 2, tail // 2, lambda step: double(2 * step, False))
    loop(tail // 2, steps // 2, lambda step: double(2 * step, True))

    whole = xb.at[:, pl.ds(0, part), :]
    for sem in (x_send, f_send):
        pltpu.make_async_copy(whole, whole, sem.at[0]).wait()
    for j in range(blocks):
        hid[:, j * NC:(j + 1) * NC] = (jax.nn.silu(acc_g[j]) * acc_u[j]).astype(BF16)

    def finish(n):
        for sub in range(PER):
            @pl.when(n < units)
            def _():
                slot = slot_down(n)
                if sub == 0:
                    wait_w(slot)
                cols = w[slot, :, :, 2 * SUB * sub:2 * SUB * (sub + 1)].reshape(half_ff, 2 * SUB)
                term = jnp.dot(hid[...], cols, preferred_element_type=F32)
                a_out(n, sub)[...] = term[:, SUB:].astype(BF16)
                keep(n, sub)[...] = term[:, :SUB]
                a_copy(n, sub).start()
                if sub == PER - 1:
                    @pl.when(n + SLOTS < units)
                    def _():
                        load_down(n + SLOTS, slot)

            b = n - LAG_B // PER

            @pl.when((b >= 0) & (b < units))
            def _():
                a_copy(b, sub).wait_recv()
                total = keep(b, sub)[...] + a_in[PER * b + sub].astype(F32)
                b_out(b, sub)[...] = total[rows:].astype(BF16)
                mine(b, sub)[...] = total[:rows]
                b_copy(b, sub).start()

            c = n - LAG_C // PER

            @pl.when((c >= 0) & (c < units))
            def _():
                b_copy(c, sub).wait_recv()
                c_out(c, sub)[...] = (mine(c, sub)[...] + b_in[PER * c + sub].astype(F32)).astype(BF16)
                c_copy(c, sub).start()

            d = n - LAG_D // PER

            @pl.when(d >= 0)
            def _():
                c_copy(d, sub).wait_recv()
                m = PER * d + sub
                d_cols(d, sub)[...] = (c_out(d, sub)[...].astype(F32) + c_in[m].astype(F32)).astype(BF16)
                d_copy(d, sub).start()

    loop(0, units + LAG_D // PER, finish)

    whole = xb.at[:, :, pl.ds(0, PER * SUB)]
    pltpu.make_async_copy(whole, whole, a_send.at[0]).wait()
    whole = xb.at[:, pl.ds(0, rows), pl.ds(0, PER * SUB)]
    for sem in (b_send, c_send, d_send, d_recv):
        pltpu.make_async_copy(whole, whole, sem.at[0]).wait()


def solution(mesh):
    def step(x, w_gate, w_up, w_down):
        rows, depth = x.shape
        ff = w_gate.shape[1]
        blocks = ff // 2 // NC
        steps = depth // KC
        pieces = depth // (2 * SUB)
        waves = SINGLES + (steps - SINGLES) // 2
        dma = pltpu.SemaphoreType.DMA
        hbm = pl.BlockSpec(memory_space=pl.ANY)
        return pl.pallas_call(
            kernel,
            out_shape=pltpu.VMEM((rows, depth), BF16),
            in_specs=[hbm] * 4,
            out_specs=pl.BlockSpec(memory_space=pltpu.VMEM),
            scratch_shapes=[
                pltpu.VMEM((steps, 2 * rows, KC), BF16),
                pltpu.VMEM((SLOTS, blocks, KC, NC), BF16),
                pltpu.VMEM((blocks, 2 * rows, NC), F32),
                pltpu.VMEM((blocks, 2 * rows, NC), F32),
                pltpu.VMEM((2 * rows, blocks * NC), BF16),
                pltpu.VMEM((pieces, 2 * rows, SUB), BF16),
                pltpu.VMEM((pieces, rows, SUB), BF16),
                pltpu.VMEM((pieces, rows, SUB), BF16),
                dma((2,)), dma((1,)), dma((waves,)), dma((1,)), dma((waves,)), dma((SLOTS,)),
                dma((1,)), dma((RING_A,)), dma((1,)), dma((RING_B,)), dma((1,)), dma((RING_C,)),
                dma((1,)), dma((1,)),
            ],
            compiler_params=pltpu.CompilerParams(
                collective_id=0, has_side_effects=True, vmem_limit_bytes=61_000_000),
        )(x, w_gate, w_up, w_down.reshape(ff // NC, NC, depth))

    return jax.shard_map(
        step,
        mesh=mesh,
        in_specs=(P("dp", None), P(None, "tp"), P(None, "tp"), P("tp", None)),
        out_specs=P("dp", None),
        check_vma=False,
    )
```

```python
import functools

import jax
import jax.numpy as jnp
from jax import lax
from jax.experimental import pallas as pl
from jax.experimental.pallas import tpu as pltpu
from jax.sharding import PartitionSpec as P

MESH = pl.DeviceIdType.MESH
F32 = jnp.float32
BF16 = jnp.bfloat16

KC = 512
NC = 512
SUB = 128
PER = NC // (2 * SUB)
SLOTS = 10
EARLY = 3
SINGLES = 8
LAG_B, LAG_C, LAG_D = 1, 4, 7
RING_A, RING_B, RING_C = 8, 16, 16


def kernel(
    x_ref, wg_ref, wu_ref, wd_ref, y_ref,
    xb, w, acc_g, acc_u, hid, a_in, b_in, c_in,
    x_load, x_send, x_recv, f_send, f_recv, w_sem,
    a_send, a_recv, b_send, b_recv, c_send, c_recv, d_send, d_recv,
):
    rows, depth = x_ref.shape
    steps = depth // KC
    blocks = w.shape[1]
    half_ff = blocks * NC
    side = depth // 2
    units = depth // NC
    part = rows // 2
    both = (0, 2 * rows)

    dp, tp = lax.axis_index("dp"), lax.axis_index("tp")
    core = lax.rem(tp, 2)
    over_core = {"dp": dp, "tp": tp + 1 - 2 * core}
    over_y = {"dp": 1 - dp, "tp": tp}
    over_x = {"dp": dp, "tp": lax.rem(tp + 2, 4)}

    def load_x(s):
        cols = pl.ds(pl.multiple_of(s * KC, KC), KC)
        which = (s >= SINGLES).astype(jnp.int32)
        return pltpu.make_async_copy(x_ref.at[:, cols], xb.at[s, pl.ds(0, rows), :], x_load.at[which])

    def loaded_x(first, count, which):
        ref = xb.at[pl.ds(first, count), pl.ds(0, rows), :]
        pltpu.make_async_copy(ref, ref, x_load.at[which]).wait()

    def x_part(base, s, count):
        return xb.at[pl.ds(s, count), pl.ds(pl.multiple_of(base + part * core, part), part), :]

    def x_sem(s, count):
        return s if count == 1 else SINGLES + (s - SINGLES) // 2

    def send_x(s, count):
        return pltpu.make_async_remote_copy(
            x_part(0, s, count), x_part(rows, s, count), x_send.at[0], x_recv.at[x_sem(s, count)],
            device_id=over_y, device_id_type=MESH)

    def forward_x(s, count):
        ref = x_part(rows, s, count)
        return pltpu.make_async_remote_copy(
            ref, ref, f_send.at[0], f_recv.at[x_sem(s, count)], device_id=over_core, device_id_type=MESH)

    def load_in(src_ref, s, slot):
        for j in range(blocks):
            cols = pl.ds(pl.multiple_of(half_ff * dp + j * NC, NC), NC)
            pltpu.make_async_copy(
                src_ref.at[pl.ds(pl.multiple_of(s * KC, KC), KC), cols], w.at[slot, j], w_sem.at[slot]).start()

    def load_down(n, slot):
        for sub in range(PER):
            for i, owner in enumerate((core, 1 - core)):
                cols = pl.ds(pl.multiple_of(side * owner + PER * SUB * n + SUB * sub, SUB), SUB)
                pltpu.make_async_copy(
                    wd_ref.at[pl.ds(blocks * dp, blocks), :, cols],
                    w.at[slot, :, :, pl.ds((2 * sub + i) * SUB, SUB)], w_sem.at[slot]).start()

    def wait_w(slot):
        pltpu.make_async_copy(w.at[slot], w.at[slot], w_sem.at[slot]).wait()

    def a_out(n, sub):
        return xb.at[n, :, pl.ds(2 * SUB * sub, SUB)]

    def b_out(n, sub):
        return xb.at[n, pl.ds(0, rows), pl.ds(2 * SUB * sub + SUB, SUB)]

    def c_out(n, sub):
        return xb.at[n, pl.ds(rows, rows), pl.ds(2 * SUB * sub + SUB, SUB)]

    def keep(n, sub):
        return acc_u.at[lax.rem(n, blocks), :, pl.ds(SUB * sub, SUB)]

    def mine(n, sub):
        return acc_g.at[lax.rem(n, blocks), pl.ds(0, rows), pl.ds(SUB * sub, SUB)]

    def a_copy(n, sub):
        m = PER * n + sub
        return pltpu.make_async_remote_copy(
            a_out(n, sub), a_in.at[m], a_send.at[0], a_recv.at[lax.rem(m, RING_A)],
            device_id=over_core, device_id_type=MESH)

    def b_copy(n, sub):
        m = PER * n + sub
        return pltpu.make_async_remote_copy(
            b_out(n, sub), b_in.at[m], b_send.at[0], b_recv.at[lax.rem(m, RING_B)],
            device_id=over_y, device_id_type=MESH)

    def c_copy(n, sub):
        m = PER * n + sub
        return pltpu.make_async_remote_copy(
            c_out(n, sub), c_in.at[m], c_send.at[0], c_recv.at[lax.rem(m, RING_C)],
            device_id=over_x, device_id_type=MESH)

    def d_cols(n, sub):
        return y_ref.at[:, pl.ds(pl.multiple_of(side * core + PER * SUB * n + SUB * sub, SUB), SUB)]

    def d_copy(n, sub):
        ref = d_cols(n, sub)
        return pltpu.make_async_remote_copy(
            ref, ref, d_send.at[0], d_recv.at[0], device_id=over_core, device_id_type=MESH)

    def loop(lo, hi, body):
        def run(i, carry):
            body(i)
            return carry

        lax.fori_loop(lo, hi, run, 0)

    barrier = pltpu.get_barrier_semaphore()
    for other in (over_core, over_y, over_x):
        pl.semaphore_signal(barrier, inc=1, device_id=other, device_id_type=MESH)
    loop(0, steps, lambda s: load_x(s).start())

    ins = ((wg_ref, acc_g), (wu_ref, acc_u))

    def slot_in(s, which):
        return lax.rem(2 * s + which, SLOTS)

    def slot_down(n):
        return lax.rem(2 * steps + n, SLOTS)

    for s in range(SLOTS // 2):
        for which in range(2):
            load_in(ins[which][0], s, slot_in(s, which))
    acc_g[...] = jnp.zeros_like(acc_g)
    acc_u[...] = jnp.zeros_like(acc_u)
    pl.semaphore_wait(barrier, 3)

    loaded_x(0, SINGLES, 0)
    loop(0, SINGLES, lambda s: send_x(s, 1).start())
    loaded_x(SINGLES, steps - SINGLES, 1)
    loop(SINGLES // 2, steps // 2, lambda step: send_x(2 * step, 2).start())

    def project(s, span, wait=True, each=False, refill=None):
        lo, size = span
        if wait and not each:
            for which in range(2):
                wait_w(slot_in(s, which))
        for which, (src_ref, acc) in enumerate(ins):
            slot = slot_in(s, which)
            if each:
                wait_w(slot)
            for j in range(blocks):
                acc[j, lo:lo + size, :] += jnp.dot(
                    xb[s, lo:lo + size, :], w[slot, j], preferred_element_type=F32)
            ahead = s + SLOTS // 2
            if refill == "in":
                load_in(src_ref, ahead, slot)
            elif refill == "down":
                load_down(2 * (ahead - steps) + which, slot)

    def take_x(s, count):
        send_x(s, count).wait_recv()
        forward_x(s, count).start()

    def own(s):
        project(s, (0, rows), each=True)

        @pl.when(s > 0)
        def _():
            take_x(s - 1, 1)

    loop(0, EARLY, own)

    def late(s):
        forward_x(s, 1).wait_recv()
        project(s, (rows, rows), wait=False, refill="in")
        take_x(s + EARLY - 1, 1)

    loop(0, EARLY, late)

    def single(s):
        @pl.when(s + 2 < SINGLES)
        def _():
            take_x(s + 2, 1)

        @pl.when(s + 2 == SINGLES)
        def _():
            take_x(SINGLES, 2)

        forward_x(s, 1).wait_recv()
        project(s, both, refill="in")

    loop(EARLY, SINGLES, single)

    def paired(s, refill):
        even = lax.rem(s, 2) == 0

        @pl.when(even & (s + 2 < steps))
        def _():
            take_x(s + 2, 2)

        @pl.when(even)
        def _():
            forward_x(s, 2).wait_recv()

        project(s, both, refill=refill)

    loop(SINGLES, steps - SLOTS // 2, lambda s: paired(s, "in"))
    loop(steps - SLOTS // 2, steps, lambda s: paired(s, "down"))

    whole = xb.at[:, pl.ds(0, part), :]
    for sem in (x_send, f_send):
        pltpu.make_async_copy(whole, whole, sem.at[0]).wait()
    def down(n):
        term = jnp.dot(hid[...], w[slot_down(n)].reshape(half_ff, NC), preferred_element_type=F32)
        for sub in range(PER):
            lo = 2 * SUB * sub
            a_out(n, sub)[...] = term[:, lo + SUB:lo + 2 * SUB].astype(BF16)
            keep(n, sub)[...] = term[:, lo:lo + SUB]
        for sub in range(PER):
            a_copy(n, sub).start()

    wait_w(slot_down(0))
    for j in range(blocks):
        hid[:, j * NC:(j + 1) * NC] = (jax.nn.silu(acc_g[j]) * acc_u[j]).astype(BF16)
    down(0)
    load_down(SLOTS, slot_down(0))

    def finish(n):
        @pl.when(n < units)
        def _():
            wait_w(slot_down(n))
            down(n)

            @pl.when(n + SLOTS < units)
            def _():
                load_down(n + SLOTS, slot_down(n))

        b = n - LAG_B

        @pl.when((b >= 0) & (b < units))
        def _():
            for sub in range(PER):
                a_copy(b, sub).wait_recv()
                total = keep(b, sub)[...] + a_in[PER * b + sub].astype(F32)
                b_out(b, sub)[...] = total[rows:].astype(BF16)
                mine(b, sub)[...] = total[:rows]
                b_copy(b, sub).start()

        c = n - LAG_C

        @pl.when((c >= 0) & (c < units))
        def _():
            for sub in range(PER):
                b_copy(c, sub).wait_recv()
                c_out(c, sub)[...] = (mine(c, sub)[...] + b_in[PER * c + sub].astype(F32)).astype(BF16)
                c_copy(c, sub).start()

        d = n - LAG_D

        @pl.when(d >= 0)
        def _():
            for sub in range(PER):
                c_copy(d, sub).wait_recv()
                m = PER * d + sub
                d_cols(d, sub)[...] = (c_out(d, sub)[...].astype(F32) + c_in[m].astype(F32)).astype(BF16)
                d_copy(d, sub).start()

    loop(1, units + LAG_D, finish)

    whole = xb.at[:, :, pl.ds(0, PER * SUB)]
    pltpu.make_async_copy(whole, whole, a_send.at[0]).wait()
    whole = xb.at[:, pl.ds(0, rows), pl.ds(0, PER * SUB)]
    for sem in (b_send, c_send, d_send, d_recv):
        pltpu.make_async_copy(whole, whole, sem.at[0]).wait()


def solution(mesh):
    def step(x, w_gate, w_up, w_down):
        rows, depth = x.shape
        ff = w_gate.shape[1]
        blocks = ff // 2 // NC
        steps = depth // KC
        pieces = depth // (2 * SUB)
        waves = SINGLES + (steps - SINGLES) // 2
        dma = pltpu.SemaphoreType.DMA
        hbm = pl.BlockSpec(memory_space=pl.ANY)
        return pl.pallas_call(
            kernel,
            out_shape=pltpu.VMEM((rows, depth), BF16),
            in_specs=[hbm] * 4,
            out_specs=pl.BlockSpec(memory_space=pltpu.VMEM),
            scratch_shapes=[
                pltpu.VMEM((steps, 2 * rows, KC), BF16),
                pltpu.VMEM((SLOTS, blocks, KC, NC), BF16),
                pltpu.VMEM((blocks, 2 * rows, NC), F32),
                pltpu.VMEM((blocks, 2 * rows, NC), F32),
                pltpu.VMEM((2 * rows, blocks * NC), BF16),
                pltpu.VMEM((pieces, 2 * rows, SUB), BF16),
                pltpu.VMEM((pieces, rows, SUB), BF16),
                pltpu.VMEM((pieces, rows, SUB), BF16),
                dma((2,)), dma((1,)), dma((waves,)), dma((1,)), dma((waves,)), dma((SLOTS,)),
                dma((1,)), dma((RING_A,)), dma((1,)), dma((RING_B,)), dma((1,)), dma((RING_C,)),
                dma((1,)), dma((1,)),
            ],
            compiler_params=pltpu.CompilerParams(
                collective_id=0, has_side_effects=True, vmem_limit_bytes=61_000_000),
        )(x, w_gate, w_up, w_down.reshape(ff // NC, NC, depth))

    return jax.shard_map(
        step,
        mesh=mesh,
        in_specs=(P("dp", None), P(None, "tp"), P(None, "tp"), P("tp", None)),
        out_specs=P("dp", None),
        check_vma=False,
    )
```

```python
import functools

import jax
import jax.numpy as jnp
from jax import lax
from jax.experimental import pallas as pl
from jax.experimental.pallas import tpu as pltpu
from jax.sharding import PartitionSpec as P

MESH = pl.DeviceIdType.MESH
F32 = jnp.float32
BF16 = jnp.bfloat16

KC = 512
NC = 512
SUB = 128
PER = NC // (2 * SUB)
SLOTS = 10
EARLY = 2
SINGLES = 8
LAG_B, LAG_C, LAG_D = 1, 4, 7
RING_A, RING_B, RING_C = 8, 16, 16


def kernel(
    x_ref, wg_ref, wu_ref, wd_ref, y_ref,
    xb, w, acc_g, acc_u, hid, a_in, b_in, c_in,
    x_load, x_send, x_recv, f_send, f_recv, w_sem,
    a_send, a_recv, b_send, b_recv, c_send, c_recv, d_send, d_recv,
):
    rows, depth = x_ref.shape
    steps = depth // KC
    blocks = w.shape[1]
    half_ff = blocks * NC
    side = depth // 2
    units = depth // NC
    part = rows // 2
    both = (0, 2 * rows)

    dp, tp = lax.axis_index("dp"), lax.axis_index("tp")
    core = lax.rem(tp, 2)
    over_core = {"dp": dp, "tp": tp + 1 - 2 * core}
    over_y = {"dp": 1 - dp, "tp": tp}
    over_x = {"dp": dp, "tp": lax.rem(tp + 2, 4)}

    def load_x(s):
        cols = pl.ds(pl.multiple_of(s * KC, KC), KC)
        which = (s >= SINGLES).astype(jnp.int32)
        return pltpu.make_async_copy(x_ref.at[:, cols], xb.at[s, pl.ds(0, rows), :], x_load.at[which])

    def loaded_x(first, count, which):
        ref = xb.at[pl.ds(first, count), pl.ds(0, rows), :]
        pltpu.make_async_copy(ref, ref, x_load.at[which]).wait()

    def x_part(base, s, count):
        return xb.at[pl.ds(s, count), pl.ds(pl.multiple_of(base + part * core, part), part), :]

    def x_sem(s, count):
        return s if count == 1 else SINGLES + (s - SINGLES) // 2

    def send_x(s, count):
        return pltpu.make_async_remote_copy(
            x_part(0, s, count), x_part(rows, s, count), x_send.at[0], x_recv.at[x_sem(s, count)],
            device_id=over_y, device_id_type=MESH)

    def forward_x(s, count):
        ref = x_part(rows, s, count)
        return pltpu.make_async_remote_copy(
            ref, ref, f_send.at[0], f_recv.at[x_sem(s, count)], device_id=over_core, device_id_type=MESH)

    def load_in(src_ref, s, slot):
        for j in range(blocks):
            cols = pl.ds(pl.multiple_of(half_ff * dp + j * NC, NC), NC)
            pltpu.make_async_copy(
                src_ref.at[pl.ds(pl.multiple_of(s * KC, KC), KC), cols], w.at[slot, j], w_sem.at[slot]).start()

    def load_down(n, slot):
        for sub in range(PER):
            for i, owner in enumerate((core, 1 - core)):
                cols = pl.ds(pl.multiple_of(side * owner + PER * SUB * n + SUB * sub, SUB), SUB)
                pltpu.make_async_copy(
                    wd_ref.at[pl.ds(blocks * dp, blocks), :, cols],
                    w.at[slot, :, :, pl.ds((2 * sub + i) * SUB, SUB)], w_sem.at[slot]).start()

    def wait_w(slot):
        pltpu.make_async_copy(w.at[slot], w.at[slot], w_sem.at[slot]).wait()

    def a_out(n, sub):
        return xb.at[n, :, pl.ds(2 * SUB * sub, SUB)]

    def b_out(n, sub):
        return xb.at[n, pl.ds(0, rows), pl.ds(2 * SUB * sub + SUB, SUB)]

    def c_out(n, sub):
        return xb.at[n, pl.ds(rows, rows), pl.ds(2 * SUB * sub + SUB, SUB)]

    def keep(n, sub):
        return acc_u.at[lax.rem(n, blocks), :, pl.ds(SUB * sub, SUB)]

    def mine(n, sub):
        return acc_g.at[lax.rem(n, blocks), pl.ds(0, rows), pl.ds(SUB * sub, SUB)]

    def a_copy(n, sub):
        m = PER * n + sub
        return pltpu.make_async_remote_copy(
            a_out(n, sub), a_in.at[m], a_send.at[0], a_recv.at[lax.rem(m, RING_A)],
            device_id=over_core, device_id_type=MESH)

    def b_copy(n, sub):
        m = PER * n + sub
        return pltpu.make_async_remote_copy(
            b_out(n, sub), b_in.at[m], b_send.at[0], b_recv.at[lax.rem(m, RING_B)],
            device_id=over_y, device_id_type=MESH)

    def c_copy(n, sub):
        m = PER * n + sub
        return pltpu.make_async_remote_copy(
            c_out(n, sub), c_in.at[m], c_send.at[0], c_recv.at[lax.rem(m, RING_C)],
            device_id=over_x, device_id_type=MESH)

    def d_cols(n, sub):
        return y_ref.at[:, pl.ds(pl.multiple_of(side * core + PER * SUB * n + SUB * sub, SUB), SUB)]

    def d_copy(n, sub):
        ref = d_cols(n, sub)
        return pltpu.make_async_remote_copy(
            ref, ref, d_send.at[0], d_recv.at[0], device_id=over_core, device_id_type=MESH)

    def loop(lo, hi, body):
        def run(i, carry):
            body(i)
            return carry

        lax.fori_loop(lo, hi, run, 0)

    barrier = pltpu.get_barrier_semaphore()
    for other in (over_core, over_y, over_x):
        pl.semaphore_signal(barrier, inc=1, device_id=other, device_id_type=MESH)
    loop(0, steps, lambda s: load_x(s).start())

    ins = ((wg_ref, acc_g), (wu_ref, acc_u))

    def slot_in(s, which):
        return lax.rem(2 * s + which, SLOTS)

    def slot_down(n):
        return lax.rem(2 * steps + n, SLOTS)

    for s in range(SLOTS // 2):
        for which in range(2):
            load_in(ins[which][0], s, slot_in(s, which))
    acc_g[...] = jnp.zeros_like(acc_g)
    acc_u[...] = jnp.zeros_like(acc_u)
    pl.semaphore_wait(barrier, 3)

    loaded_x(0, SINGLES, 0)
    loop(0, SINGLES, lambda s: send_x(s, 1).start())
    loaded_x(SINGLES, steps - SINGLES, 1)
    loop(SINGLES // 2, steps // 2, lambda step: send_x(2 * step, 2).start())

    def project(s, span, wait=True, each=False, refill=None):
        lo, size = span
        if wait and not each:
            for which in range(2):
                wait_w(slot_in(s, which))
        for which, (src_ref, acc) in enumerate(ins):
            slot = slot_in(s, which)
            if each:
                wait_w(slot)
            for j in range(blocks):
                acc[j, lo:lo + size, :] += jnp.dot(
                    xb[s, lo:lo + size, :], w[slot, j], preferred_element_type=F32)
            ahead = s + SLOTS // 2
            if refill == "in":
                load_in(src_ref, ahead, slot)
            elif refill == "down":
                load_down(2 * (ahead - steps) + which, slot)

    def take_x(s, count):
        send_x(s, count).wait_recv()
        forward_x(s, count).start()

    def own(s):
        project(s, (0, rows), each=True)

        @pl.when(s > 0)
        def _():
            take_x(s - 1, 1)

    loop(0, EARLY, own)

    def late(s):
        forward_x(s, 1).wait_recv()
        project(s, (rows, rows), wait=False, refill="in")
        take_x(s + EARLY - 1, 1)

    loop(0, EARLY, late)

    def single(s):
        @pl.when(s + EARLY - 1 < SINGLES)
        def _():
            take_x(s + EARLY - 1, 1)

        @pl.when(s + EARLY - 1 == SINGLES)
        def _():
            take_x(SINGLES, 2)

        forward_x(s, 1).wait_recv()
        project(s, both, refill="in")

    loop(EARLY, SINGLES, single)

    def paired(s, refill):
        even = lax.rem(s, 2) == 0

        @pl.when(even & (s + 2 < steps))
        def _():
            take_x(s + 2, 2)

        @pl.when(even)
        def _():
            forward_x(s, 2).wait_recv()

        project(s, both, refill=refill)

    loop(SINGLES, steps - SLOTS // 2, lambda s: paired(s, "in"))
    loop(steps - SLOTS // 2, steps, lambda s: paired(s, "down"))

    whole = xb.at[:, pl.ds(0, part), :]
    for sem in (x_send, f_send):
        pltpu.make_async_copy(whole, whole, sem.at[0]).wait()
    def down(n):
        term = jnp.dot(hid[...], w[slot_down(n)].reshape(half_ff, NC), preferred_element_type=F32)
        for sub in range(PER):
            lo = 2 * SUB * sub
            a_out(n, sub)[...] = term[:, lo + SUB:lo + 2 * SUB].astype(BF16)
            keep(n, sub)[...] = term[:, lo:lo + SUB]
        for sub in range(PER):
            a_copy(n, sub).start()

    wait_w(slot_down(0))
    for j in range(blocks):
        hid[:, j * NC:(j + 1) * NC] = (jax.nn.silu(acc_g[j]) * acc_u[j]).astype(BF16)
    down(0)
    load_down(SLOTS, slot_down(0))

    def finish(n):
        @pl.when(n < units)
        def _():
            wait_w(slot_down(n))
            down(n)

            @pl.when(n + SLOTS < units)
            def _():
                load_down(n + SLOTS, slot_down(n))

        b = n - LAG_B

        @pl.when((b >= 0) & (b < units))
        def _():
            for sub in range(PER):
                a_copy(b, sub).wait_recv()
                total = keep(b, sub)[...] + a_in[PER * b + sub].astype(F32)
                b_out(b, sub)[...] = total[rows:].astype(BF16)
                mine(b, sub)[...] = total[:rows]
                b_copy(b, sub).start()

        c = n - LAG_C

        @pl.when((c >= 0) & (c < units))
        def _():
            for sub in range(PER):
                b_copy(c, sub).wait_recv()
                c_out(c, sub)[...] = (mine(c, sub)[...] + b_in[PER * c + sub].astype(F32)).astype(BF16)
                c_copy(c, sub).start()

        d = n - LAG_D

        @pl.when(d >= 0)
        def _():
            for sub in range(PER):
                c_copy(d, sub).wait_recv()
                m = PER * d + sub
                d_cols(d, sub)[...] = (c_out(d, sub)[...].astype(F32) + c_in[m].astype(F32)).astype(BF16)
                d_copy(d, sub).start()

    loop(1, units + LAG_D, finish)

    whole = xb.at[:, :, pl.ds(0, PER * SUB)]
    pltpu.make_async_copy(whole, whole, a_send.at[0]).wait()
    whole = xb.at[:, pl.ds(0, rows), pl.ds(0, PER * SUB)]
    for sem in (b_send, c_send, d_send, d_recv):
        pltpu.make_async_copy(whole, whole, sem.at[0]).wait()


def solution(mesh):
    def step(x, w_gate, w_up, w_down):
        rows, depth = x.shape
        ff = w_gate.shape[1]
        blocks = ff // 2 // NC
        steps = depth // KC
        pieces = depth // (2 * SUB)
        waves = SINGLES + (steps - SINGLES) // 2
        dma = pltpu.SemaphoreType.DMA
        hbm = pl.BlockSpec(memory_space=pl.ANY)
        return pl.pallas_call(
            kernel,
            out_shape=pltpu.VMEM((rows, depth), BF16),
            in_specs=[hbm] * 4,
            out_specs=pl.BlockSpec(memory_space=pltpu.VMEM),
            scratch_shapes=[
                pltpu.VMEM((steps, 2 * rows, KC), BF16),
                pltpu.VMEM((SLOTS, blocks, KC, NC), BF16),
                pltpu.VMEM((blocks, 2 * rows, NC), F32),
                pltpu.VMEM((blocks, 2 * rows, NC), F32),
                pltpu.VMEM((2 * rows, blocks * NC), BF16),
                pltpu.VMEM((pieces, 2 * rows, SUB), BF16),
                pltpu.VMEM((pieces, rows, SUB), BF16),
                pltpu.VMEM((pieces, rows, SUB), BF16),
                dma((2,)), dma((1,)), dma((waves,)), dma((1,)), dma((waves,)), dma((SLOTS,)),
                dma((1,)), dma((RING_A,)), dma((1,)), dma((RING_B,)), dma((1,)), dma((RING_C,)),
                dma((1,)), dma((1,)),
            ],
            compiler_params=pltpu.CompilerParams(
                collective_id=0, has_side_effects=True, vmem_limit_bytes=61_000_000),
        )(x, w_gate, w_up, w_down.reshape(ff // NC, NC, depth))

    return jax.shard_map(
        step,
        mesh=mesh,
        in_specs=(P("dp", None), P(None, "tp"), P(None, "tp"), P("tp", None)),
        out_specs=P("dp", None),
        check_vma=False,
    )
```
